8 devices in a mesh: dp: 1 (over z), tp: 2 (over y), cp: 4 (over x, core).
Axes of the slice: x: 2, y: 2, z: 1, core: 2. Of those that a mesh axis runs over, the one named last changes fastest.
Arguments:
- x: bfloat16 [4096, 4096], P(('dp', 'cp'))
- kc: bfloat16 [8192, 32, 128], P(('dp', 'cp'), 'tp')
- vc: bfloat16 [8192, 32, 128], P(('dp', 'cp'), 'tp')
- wq: bfloat16 [4096, 4096], P(None, 'tp')
- wk: bfloat16 [4096, 4096], P(None, 'tp')
- wv: bfloat16 [4096, 4096], P(None, 'tp')
- wo: bfloat16 [4096, 4096], P('tp')
Outputs:
- output 1: bfloat16 [4096, 4096], P(('dp', 'cp'), 'tp')
- output 2: bfloat16 [4096, 32, 128], P(('dp', 'cp'), 'tp')
- output 3: bfloat16 [4096, 32, 128], P(('dp', 'cp'), 'tp')
All inputs are finite; a program needn't handle non-finite values.
Results may differ from the reference program's by a relative error of at most 0.011.
Values are sent between devices in bfloat16 or wider.
A program may use at most 1 GiB of HBM per device.

```python
import math
import jax
import jax.numpy as jnp
from jax import lax

T = 4096
C = 8192
DM = 4096
H = 32
HKV = 32
HEAD = 128
NSEG = 8
QB = 64

G = H // HKV
SCALE = HEAD ** -0.5


def _rope(a, pos):
    half = HEAD // 2
    inv = 1.0 / (500000.0 ** (jnp.arange(half, dtype=jnp.float32) * 2.0 / HEAD))
    ang = pos.astype(jnp.float32)[:, None] * inv[None, :]
    cos = jnp.cos(ang)[:, None, :]
    sin = jnp.sin(ang)[:, None, :]
    af = a.astype(jnp.float32)
    a1 = af[..., :half]
    a2 = af[..., half:]
    return jnp.concatenate([a1 * cos - a2 * sin, a2 * cos + a1 * sin], axis=-1).astype(jnp.bfloat16)


def setup_inputs(seed: int = 0, part: int = 0) -> dict:
    shared, own = jax.random.split(jax.random.key(seed))
    own = jax.random.fold_in(own, part)
    kx, kk, kv, ks, km = jax.random.split(own, 5)
    kq, kwk, kwv, kwo = jax.random.split(shared, 4)
    seg = C // NSEG
    sig = jax.random.uniform(ks, (NSEG, HKV), jnp.float32, 0.5, 1.5)
    mu = jax.random.normal(km, (NSEG, HKV, HEAD), jnp.float32)
    kc = jax.random.normal(kk, (C, HKV, HEAD), jnp.float32) * jnp.repeat(sig, seg, axis=0)[:, :, None]
    vc = jax.random.normal(kv, (C, HKV, HEAD), jnp.float32) + jnp.repeat(mu, seg, axis=0)
    x = jax.random.normal(kx, (T, DM), jnp.float32)
    gain = math.sqrt(max(1.0, 2.0 * math.log(1.2 * C / T)))
    wq = jax.random.normal(kq, (DM, H * HEAD), jnp.float32) * DM ** -0.5
    wk = jax.random.normal(kwk, (DM, HKV * HEAD), jnp.float32) * (gain * DM ** -0.5)
    wv = jax.random.normal(kwv, (DM, HKV * HEAD), jnp.float32) * DM ** -0.5
    wo = jax.random.normal(kwo, (H * HEAD, DM), jnp.float32) * (H * HEAD) ** -0.5
    bf = jnp.bfloat16
    return {'x': x.astype(bf), 'kc': kc.astype(bf), 'vc': vc.astype(bf), 'wq': wq.astype(bf),
            'wk': wk.astype(bf), 'wv': wv.astype(bf), 'wo': wo.astype(bf)}


def reference(x, kc, vc, wq, wk, wv, wo):
    f32 = jnp.float32
    pos = C + jnp.arange(T, dtype=jnp.int32)
    q = jnp.dot(x, wq, preferred_element_type=f32).astype(jnp.bfloat16).reshape(T, H, HEAD)
    k = jnp.dot(x, wk, preferred_element_type=f32).astype(jnp.bfloat16).reshape(T, HKV, HEAD)
    v = jnp.dot(x, wv, preferred_element_type=f32).astype(jnp.bfloat16).reshape(T, HKV, HEAD)
    q = _rope(q, pos).reshape(T // QB, QB, HKV, G, HEAD)
    k = _rope(k, pos)
    keys = jnp.concatenate([kc, k], axis=0).astype(f32)
    vals = jnp.concatenate([vc, v], axis=0).astype(f32)
    kpos = jnp.arange(C + T)

    def qblock(args):
        qb, i = args
        qb = qb.astype(f32)
        mask = kpos[None, :] <= (C + i * QB + jnp.arange(QB))[:, None]

        def head(j):
            s = jnp.einsum('qgd,kd->qgk', qb[:, j], keys[:, j]) * SCALE
            s = jnp.where(mask[:, None, :], s, -jnp.inf)
            p = jnp.exp(s - jnp.max(s, axis=-1, keepdims=True))
            l = jnp.sum(p, axis=-1, keepdims=True)
            o = jnp.einsum('qgk,kd->qgd', p.astype(jnp.bfloat16).astype(f32), vals[:, j])
            return o / l

        o = lax.map(head, jnp.arange(HKV))
        return o.transpose(1, 0, 2, 3).reshape(QB, H * HEAD)

    o = lax.map(qblock, (q, jnp.arange(T // QB))).reshape(T, H * HEAD)
    y = jnp.dot(o.astype(jnp.bfloat16), wo, preferred_element_type=f32).astype(jnp.bfloat16)
    return y, k, v
```

```python
import functools
import math

import jax
import jax.numpy as jnp
from jax import lax
from jax.experimental import pallas as pl
from jax.experimental.pallas import tpu as pltpu
from jax.sharding import PartitionSpec as P


THETA = 500000.0
F32 = jnp.float32
BF16 = jnp.bfloat16
NEG = -1e30
VMEM = 60 * 1024 * 1024
ORDER = (('R', 0, 4), ('R', 4, 4), ('L', 0, 8), ('R', 8, 4), ('R', 12, 4), ('M', 0, 8), ('L', 8, 8), ('M', 8, 4),
         ('M', 12, 4), ('Y', 0, 12), ('Z', 12, 4))


def _after(a, *deps):
    return lax.optimization_barrier((a, *deps))[0]


def _tables(pos, d):
    half = d // 2
    inv = 1.0 / (THETA ** (jnp.arange(half, dtype=F32) * 2.0 / d))
    ang = pos.astype(F32)[:, None] * inv[None, :]
    cos, sin = jnp.cos(ang), jnp.sin(ang)
    return jnp.concatenate([cos, cos], axis=1), jnp.concatenate([-sin, sin], axis=1)


def _proj(x, w, tabs, col0, ncols, d, bn=256):
    m, k = x.shape

    def kern(*refs):
        if tabs is None:
            x_ref, w_ref, o_ref = refs
        else:
            x_ref, w_ref, c_ref, s_ref, o_ref = refs
        r = jnp.dot(x_ref[...], w_ref[...], preferred_element_type=F32).astype(BF16)
        if tabs is None:
            o_ref[...] = r
        else:
            for h in range(bn // d):
                a = r[:, h * d:(h + 1) * d].astype(F32)
                o_ref[:, h * d:(h + 1) * d] = (a * c_ref[...] + pltpu.roll(a, d // 2, 1) * s_ref[...]).astype(BF16)

    full = lambda s: pl.BlockSpec(s, lambda j: (0, 0))
    j0 = col0 // bn
    extra = [] if tabs is None else [full((m, d)), full((m, d))]
    return pl.pallas_call(
        kern,
        grid=(ncols // bn,),
        in_specs=[full((m, k)), pl.BlockSpec((k, bn), lambda j: (0, j + j0))] + extra,
        out_specs=pl.BlockSpec((m, bn), lambda j: (0, j)),
        out_shape=jax.ShapeDtypeStruct((m, ncols), BF16),
        compiler_params=pltpu.CompilerParams(vmem_limit_bytes=VMEM),
        cost_estimate=pl.CostEstimate(flops=2 * m * k * ncols, bytes_accessed=2 * (m * k + k * ncols + m * ncols),
                                      transcendentals=0),
    )(x, w, *(tabs or ()))


def _attend(flags, q, qcol, kvs, h0, nh, d, causal):
    tq = q.shape[0]
    c = kvs[0][0].shape[0]
    n = kvs[2][0].shape[0]
    m0 = 64
    hq = tq // 2
    fb = 128
    scale = (d ** -0.5) * math.log2(math.e)
    tdot = lambda a, b: lax.dot_general(a, b, (((1,), (1,)), ((), ())), preferred_element_type=F32)
    vdot = lambda a, b: lax.dot_general(a, b, (((0,), (0,)), ((), ())), preferred_element_type=F32)

    def kern(f_ref, q_ref, *refs):
        ks, vs = refs[0:4], refs[4:8]
        o_ref, l_ref, acc_sc, d_sc = refs[8:]
        qf = q_ref[...].astype(F32) * scale
        hi = qf.astype(BF16)
        q2 = jnp.concatenate([hi, (qf - hi.astype(F32)).astype(BF16)], axis=1).T

        def scores(k_ref, row, rows, q0, qn):
            kb = k_ref[row:row + rows, :]
            return jnp.dot(jnp.concatenate([kb, kb], axis=1), q2[:, q0:q0 + qn], preferred_element_type=F32)

        mc = jnp.max(scores(ks[0], 0, m0, 0, tq), axis=0, keepdims=True)

        def run(parts, den, acc):
            for a, bk, q0, qn, masked in parts:
                s = scores(ks[a], 0, bk, q0, qn)
                if masked:
                    kp = lax.broadcasted_iota(jnp.int32, (bk, qn), 0)
                    qp = lax.broadcasted_iota(jnp.int32, (bk, qn), 1) + q0
                    s = jnp.where(kp <= qp, s, NEG)
                p = jnp.exp2(s - mc[:, q0:q0 + qn])
                den[q0, qn] = den.get((q0, qn), 0) + jnp.sum(p.reshape(bk // 8, 8, qn), axis=0)
                acc[q0, qn] = acc.get((q0, qn), 0) + vdot(vs[a][:bk, :], p.astype(BF16))

        def flush(parts, first):
            den, acc = {}, {}
            run(parts, den, acc)
            for i, (q0, qn) in enumerate(den):
                if first and i == 0:
                    d_sc[:, q0:q0 + qn] = den[q0, qn]
                    acc_sc[:, q0:q0 + qn] = acc[q0, qn]
                else:
                    d_sc[:, q0:q0 + qn] += den[q0, qn]
                    acc_sc[:, q0:q0 + qn] += acc[q0, qn]

        parts = [(0, c, 0, tq, False), (1, c, 0, tq, False)]
        if causal:
            parts += [(2, hq, 0, hq, True), (2, tq, hq, hq, True)]
        flush(parts, True)

        @pl.when(f_ref[1 if causal else 0] == 1)
        def _():
            flush([(a, n, 0, tq, False) for a in ((3,) if causal else (2, 3))], False)

        def finish(den, acc, m, qs):
            o_ref[:, qs] = acc / den
            l_ref[0, :, qs] = m + jnp.log2(den)

        den = jnp.sum(d_sc[...], axis=0, keepdims=True)
        top = jnp.max(jnp.abs(acc_sc[...]), axis=0, keepdims=True)
        good = jnp.where((den < 2.0 ** 100) & (top < 2.0 ** 126), 1.0, 0.0)
        finish(den, acc_sc[...], mc, slice(None))

        @pl.when(jnp.min(good) < 0.5)
        def _():
            def qblock(i, _):
                qs = pl.ds(pl.multiple_of(i * fb, fb), fb)
                qb = q_ref[qs, :]

                def kstep(k_ref, v_ref, masked):
                    def step(j, carry):
                        m, den, acc = carry
                        rows = pl.ds(pl.multiple_of(j * fb, fb), fb)
                        s = tdot(k_ref[rows, :], qb) * scale
                        if masked:
                            kp = lax.broadcasted_iota(jnp.int32, (fb, fb), 0) + j * fb
                            qp = lax.broadcasted_iota(jnp.int32, (fb, fb), 1) + i * fb
                            s = jnp.where(kp <= qp, s, NEG)
                        mn = jnp.maximum(m, jnp.max(s, axis=0, keepdims=True))
                        al = jnp.exp2(m - mn)
                        p = jnp.exp2(s - mn)
                        return (mn, den * al + jnp.sum(p, axis=0, keepdims=True),
                                acc * al + vdot(v_ref[rows, :], p.astype(BF16)))

                    return step

                st = (jnp.full((1, fb), NEG, F32), jnp.zeros((1, fb), F32), jnp.zeros((d, fb), F32))
                for a in range(2):
                    st = lax.fori_loop(0, c // fb, kstep(ks[a], vs[a], False), st)
                own = i + 1 if causal else f_ref[0] * (n // fb)
                st = lax.fori_loop(0, own, kstep(ks[2], vs[2], causal), st)
                st = lax.fori_loop(0, f_ref[1 if causal else 0] * (n // fb), kstep(ks[3], vs[3], False), st)
                finish(st[1], st[2], st[0], qs)
                return 0

            lax.fori_loop(0, tq // fb, qblock, 0)

    kspec = lambda rows: pl.BlockSpec((rows, d), lambda h, f: (0, h + h0))
    rows = [c, c, n, n]
    keys = 2 * c + n
    return pl.pallas_call(
        kern,
        grid_spec=pltpu.PrefetchScalarGridSpec(
            num_scalar_prefetch=1,
            grid=(nh,),
            in_specs=[pl.BlockSpec((tq, d), lambda h, f: (0, h + qcol))] + [kspec(r) for r in rows] * 2,
            out_specs=[pl.BlockSpec((d, tq), lambda h, f: (h, 0)), pl.BlockSpec((1, 1, tq), lambda h, f: (h, 0, 0))],
            scratch_shapes=[pltpu.VMEM((d, tq), F32), pltpu.VMEM((8, tq), F32)],
        ),
        out_shape=[jax.ShapeDtypeStruct((nh * d, tq), F32), jax.ShapeDtypeStruct((nh, 1, tq), F32)],
        compiler_params=pltpu.CompilerParams(vmem_limit_bytes=VMEM),
        cost_estimate=pl.CostEstimate(flops=12 * tq * keys * nh * d, bytes_accessed=4 * keys * nh * d,
                                      transcendentals=tq * keys * nh),
    )(flags, q, *[kv[0] for kv in kvs], *[kv[1] for kv in kvs])


def _merge(loc, first, rem, nh, d):
    tq = loc[0].shape[1]
    sizes = [l.shape[0] for _, l in rem]
    starts = [sum(sizes[:i]) for i in range(len(sizes))]

    def kern(o1_ref, l1_ref, *refs):
        o_ref = refs[-1]
        h = pl.program_id(0)

        def one(o2_ref, l2_ref):
            a, b = l1_ref[0], l2_ref[0]
            m = jnp.maximum(a, b)
            wa, wb = jnp.exp2(a - m), jnp.exp2(b - m)
            t = 1.0 / (wa + wb)
            o_ref[...] = (o1_ref[...] * (wa * t) + o2_ref[...] * (wb * t)).astype(BF16).T

        for i, (s, n) in enumerate(zip(starts, sizes)):
            pl.when((h >= s) & (h < s + n))(functools.partial(one, refs[2 * i], refs[2 * i + 1]))

    in_specs = [pl.BlockSpec((d, tq), lambda h: (h + first, 0)), pl.BlockSpec((1, 1, tq), lambda h: (h + first, 0, 0))]
    for s, n in zip(starts, sizes):
        at = lambda h, s=s, n=n: jnp.clip(h - s, 0, n - 1)
        in_specs += [pl.BlockSpec((d, tq), lambda h, at=at: (at(h), 0)),
                     pl.BlockSpec((1, 1, tq), lambda h, at=at: (at(h), 0, 0))]
    return pl.pallas_call(
        kern,
        grid=(nh,),
        in_specs=in_specs,
        out_specs=pl.BlockSpec((tq, d), lambda h: (0, h)),
        out_shape=jax.ShapeDtypeStruct((tq, nh * d), BF16),
        compiler_params=pltpu.CompilerParams(vmem_limit_bytes=VMEM),
        cost_estimate=pl.CostEstimate(flops=2000 * tq * nh * d, bytes_accessed=10 * tq * nh * d, transcendentals=0),
    )(*loc, *[a for r in rem for a in r])


def _flatten(a, b, br=256):
    n, h, d = a.shape

    def kern(a_ref, b_ref, oa_ref, ob_ref):
        oa_ref[...] = a_ref[...].reshape(br, h * d)
        ob_ref[...] = b_ref[...].reshape(br, h * d)

    return pl.pallas_call(
        kern,
        grid=(n // br,),
        in_specs=[pl.BlockSpec((br, h, d), lambda i: (i, 0, 0))] * 2,
        out_specs=[pl.BlockSpec((br, h * d), lambda i: (i, 0))] * 2,
        out_shape=[jax.ShapeDtypeStruct((n, h * d), BF16)] * 2,
        compiler_params=pltpu.CompilerParams(vmem_limit_bytes=VMEM),
        cost_estimate=pl.CostEstimate(flops=1000 * n * h * d, bytes_accessed=8 * n * h * d, transcendentals=0),
    )(a, b)


def _out(t, terms, acc, ncols, final, bn=512):
    tl = terms[0][0].shape[0]
    nt = len(terms)

    def kern(t_ref, *refs):
        o_ref = refs[-1]
        r = None if acc is None else refs[2 * nt][...]
        for i in range(nt):
            p = jnp.dot(refs[i][...], refs[nt + i][...], preferred_element_type=F32)
            r = p if r is None else r + p
        o_ref[...] = r.astype(o_ref.dtype)

    nb = ncols // bn

    def wspec(o, row, mine):
        rows = o.shape[1]
        if mine:
            return pl.BlockSpec((rows, bn), lambda j, tt: (row // rows, j + tt[0] * nb))
        return pl.BlockSpec((rows, bn), lambda j, tt: (row // rows, j))

    ospec = pl.BlockSpec((tl, bn), lambda j, tt: (0, j))
    k = sum(o.shape[1] for o, *_ in terms)
    return pl.pallas_call(
        kern,
        grid_spec=pltpu.PrefetchScalarGridSpec(
            num_scalar_prefetch=1,
            grid=(nb,),
            in_specs=[pl.BlockSpec(o.shape, lambda j, tt: (0, 0)) for o, *_ in terms]
            + [wspec(o, row, mine) for o, _, row, mine in terms] + ([] if acc is None else [ospec]),
            out_specs=ospec,
        ),
        out_shape=jax.ShapeDtypeStruct((tl, ncols), BF16 if final else F32),
        compiler_params=pltpu.CompilerParams(vmem_limit_bytes=VMEM),
        cost_estimate=pl.CostEstimate(flops=2 * tl * k * ncols, bytes_accessed=2 * k * ncols, transcendentals=0),
    )(t, *[o for o, *_ in terms], *[w for _, w, *_ in terms], *([] if acc is None else [acc]))


def solution(mesh):
    ncp = mesh.shape['cp']
    ntp = mesh.shape['tp']
    row = P(('dp', 'cp'), None)
    cache = P(('dp', 'cp'), 'tp', None)
    col = P(None, 'tp')
    half = ncp // 2
    core = [(i, i ^ 1) for i in range(ncp)]
    chip = [(i, (i + half) % ncp) for i in range(ncp)]
    swap = [(0, 1), (1, 0)]

    def body(x, kc, vc, wq, wk, wv, wo):
        tl = x.shape[0]
        cl, hl, d = kc.shape
        w = hl * d
        r = lax.axis_index('cp')
        t = lax.axis_index('tp')
        flags = jnp.stack([(r < half).astype(jnp.int32), r % 2])
        tt = t.reshape(1)
        ncols = wo.shape[1] // ntp
        hq = hl // 2

        tabs = _tables(cl * ncp + r * tl + jnp.arange(tl, dtype=jnp.int32), d)
        qs, qr = [], []
        prev = tabs[0]
        for i in range(2):
            qs.append(_proj(x, _after(wq, prev), tabs, i * (w // 2), w // 2, d))
            prev = qs[i]
            qr.append(lax.ppermute(prev, 'cp', chip))
        kc2, vc2 = _flatten(_after(kc, prev), vc)
        kcp = lax.ppermute(kc2, 'cp', core)
        vcp = lax.ppermute(vc2, 'cp', core)
        k = _proj(x, _after(wk, vc2), tabs, 0, w, d)
        kp = lax.ppermute(k, 'cp', core)
        v = _proj(x, _after(wv, k), None, 0, w, d)
        vp = lax.ppermute(v, 'cp', core)
        wo_other = lax.ppermute(lax.dynamic_slice(_after(wo, v), (0, (1 - t) * ncols), (w, ncols)), 'tp', swap)
        kvs = [(kc2, vc2), (kcp, vcp), (k, v), (kp, vp)]

        prev, y = v, None
        rem, loc, os = {}, {}, {}
        for kind, h0, nh in ORDER:
            if kind == 'R':
                o, l = _attend(_after(flags, prev), qr[h0 // hq], h0 % hq, kvs, h0, nh, d, False)
                prev = l
            elif kind == 'L':
                loc[h0, nh] = _attend(_after(flags, prev), qs[h0 // hq], h0 % hq, kvs, h0, nh, d, True)
                prev = loc[h0, nh][1]
            elif kind == 'M':
                (l0, ln), part = next((k, p) for k, p in loc.items() if k[0] <= h0 < sum(k))
                prev = _merge((part[0], _after(part[1], prev)), h0 - l0,
                              [rem[g] for g in sorted(rem) if h0 <= g < h0 + nh], nh, d)
                os[h0] = [(prev, wo, h0 * d, True)]
            else:
                terms = sum([os[g] for g in sorted(os) if h0 <= g < h0 + nh], [])
                prev = y = _out(_after(tt, prev), terms, y, ncols, kind == 'Z')
            if kind == 'R':
                rem[h0] = lax.ppermute(o, 'cp', chip), lax.ppermute(l, 'cp', chip)
            elif kind == 'M':
                os[h0].append((lax.ppermute(prev, 'tp', swap), wo_other, h0 * d, False))
        return y, k.reshape(tl, hl, d), v.reshape(tl, hl, d)

    return jax.shard_map(body, mesh=mesh,
                         in_specs=(row, cache, cache, col, col, col, P('tp', None)),
                         out_specs=(P(('dp', 'cp'), 'tp'), cache, cache), check_vma=False)
```

```python
import functools
import math

import jax
import jax.numpy as jnp
from jax import lax
from jax.experimental import pallas as pl
from jax.experimental.pallas import tpu as pltpu
from jax.sharding import PartitionSpec as P


THETA = 500000.0
F32 = jnp.float32
BF16 = jnp.bfloat16
NEG = -1e30
VMEM = 60 * 1024 * 1024
SMALL = 32 * 1024 * 1024
ORDER = (('R', 0, 4), ('R', 4, 4), ('L', 0, 8), ('R', 8, 4), ('R', 12, 4), ('M', 0, 8), ('L', 8, 4), ('M', 8, 4),
         ('L', 12, 4), ('M', 12, 4), ('Y', 0, 12), ('Z', 12, 4))


def _after(a, *deps):
    return lax.optimization_barrier((a, *deps))[0]


def _tables(pos, d):
    half = d // 2
    inv = 1.0 / (THETA ** (jnp.arange(half, dtype=F32) * 2.0 / d))
    ang = pos.astype(F32)[:, None] * inv[None, :]
    cos, sin = jnp.cos(ang), jnp.sin(ang)
    return jnp.concatenate([cos, cos], axis=1), jnp.concatenate([-sin, sin], axis=1)


def _proj(x, w, tabs, col0, ncols, d, bn=256):
    m, k = x.shape

    def kern(*refs):
        if tabs is None:
            x_ref, w_ref, o_ref = refs
        else:
            x_ref, w_ref, c_ref, s_ref, o_ref = refs
        r = jnp.dot(x_ref[...], w_ref[...], preferred_element_type=F32).astype(BF16)
        if tabs is None:
            o_ref[...] = r
        else:
            for h in range(bn // d):
                a = r[:, h * d:(h + 1) * d].astype(F32)
                o_ref[:, h * d:(h + 1) * d] = (a * c_ref[...] + pltpu.roll(a, d // 2, 1) * s_ref[...]).astype(BF16)

    full = lambda s: pl.BlockSpec(s, lambda j: (0, 0))
    j0 = col0 // bn
    extra = [] if tabs is None else [full((m, d)), full((m, d))]
    return pl.pallas_call(
        kern,
        grid=(ncols // bn,),
        in_specs=[pl.BlockSpec(memory_space=pltpu.VMEM), pl.BlockSpec((k, bn), lambda j: (0, j + j0))] + extra,
        out_specs=pl.BlockSpec((m, bn), lambda j: (0, j)),
        out_shape=jax.ShapeDtypeStruct((m, ncols), BF16),
        compiler_params=pltpu.CompilerParams(vmem_limit_bytes=SMALL),
        cost_estimate=pl.CostEstimate(flops=2 * m * k * ncols, bytes_accessed=2 * (m * k + k * ncols + m * ncols),
                                      transcendentals=0),
    )(x, w, *(tabs or ()))


def _attend(flags, q, qcol, kvs, h0, nh, d, causal):
    tq = q.shape[0]
    c = kvs[0][0].shape[0]
    n = kvs[2][0].shape[0]
    m0 = 64
    hq = tq // 2
    fb = 128
    scale = (d ** -0.5) * math.log2(math.e)
    tdot = lambda a, b: lax.dot_general(a, b, (((1,), (1,)), ((), ())), preferred_element_type=F32)
    vdot = lambda a, b: lax.dot_general(a, b, (((0,), (0,)), ((), ())), preferred_element_type=F32)

    def kern(f_ref, q_ref, *refs):
        ks, vs = refs[0:4], refs[4:8]
        o_ref, l_ref, acc_sc, d_sc = refs[8:]
        qf = q_ref[...].astype(F32) * scale
        hi = qf.astype(BF16)
        q2 = jnp.concatenate([hi, (qf - hi.astype(F32)).astype(BF16)], axis=1).T

        def scores(k_ref, row, rows, q0, qn):
            kb = k_ref[row:row + rows, :]
            return jnp.dot(jnp.concatenate([kb, kb], axis=1), q2[:, q0:q0 + qn], preferred_element_type=F32)

        mc = jnp.max(scores(ks[0], 0, m0, 0, tq), axis=0, keepdims=True)

        def run(parts, den, acc):
            for a, bk, q0, qn, masked in parts:
                s = scores(ks[a], 0, bk, q0, qn)
                if masked:
                    kp = lax.broadcasted_iota(jnp.int32, (bk, qn), 0)
                    qp = lax.broadcasted_iota(jnp.int32, (bk, qn), 1) + q0
                    s = jnp.where(kp <= qp, s, NEG)
                p = jnp.exp2(s - mc[:, q0:q0 + qn])
                den[q0, qn] = den.get((q0, qn), 0) + jnp.sum(p.reshape(bk // 8, 8, qn), axis=0)
                acc[q0, qn] = acc.get((q0, qn), 0) + vdot(vs[a][:bk, :], p.astype(BF16))

        def flush(parts, first):
            den, acc = {}, {}
            run(parts, den, acc)
            for i, (q0, qn) in enumerate(den):
                if first and i == 0:
                    d_sc[:, q0:q0 + qn] = den[q0, qn]
                    acc_sc[:, q0:q0 + qn] = acc[q0, qn]
                else:
                    d_sc[:, q0:q0 + qn] += den[q0, qn]
                    acc_sc[:, q0:q0 + qn] += acc[q0, qn]

        parts = [(0, c, 0, tq, False), (1, c, 0, tq, False)]
        if causal:
            parts += [(2, hq, 0, hq, True), (2, tq, hq, hq, True)]
        flush(parts, True)

        @pl.when(f_ref[1 if causal else 0] == 1)
        def _():
            flush([(a, n, 0, tq, False) for a in ((3,) if causal else (2, 3))], False)

        def finish(den, acc, m, qs):
            o_ref[:, qs] = acc / den
            l_ref[0, :, qs] = m + jnp.log2(den)

        den = jnp.sum(d_sc[...], axis=0, keepdims=True)
        top = jnp.max(jnp.abs(acc_sc[...]), axis=0, keepdims=True)
        good = jnp.where((den < 2.0 ** 100) & (top < 2.0 ** 126), 1.0, 0.0)
        finish(den, acc_sc[...], mc, slice(None))

        @pl.when(jnp.min(good) < 0.5)
        def _():
            def qblock(i, _):
                qs = pl.ds(pl.multiple_of(i * fb, fb), fb)
                qb = q_ref[qs, :]

                def kstep(k_ref, v_ref, masked):
                    def step(j, carry):
                        m, den, acc = carry
                        rows = pl.ds(pl.multiple_of(j * fb, fb), fb)
                        s = tdot(k_ref[rows, :], qb) * scale
                        if masked:
                            kp = lax.broadcasted_iota(jnp.int32, (fb, fb), 0) + j * fb
                            qp = lax.broadcasted_iota(jnp.int32, (fb, fb), 1) + i * fb
                            s = jnp.where(kp <= qp, s, NEG)
                        mn = jnp.maximum(m, jnp.max(s, axis=0, keepdims=True))
                        al = jnp.exp2(m - mn)
                        p = jnp.exp2(s - mn)
                        return (mn, den * al + jnp.sum(p, axis=0, keepdims=True),
                                acc * al + vdot(v_ref[rows, :], p.astype(BF16)))

                    return step

                st = (jnp.full((1, fb), NEG, F32), jnp.zeros((1, fb), F32), jnp.zeros((d, fb), F32))
                for a in range(2):
                    st = lax.fori_loop(0, c // fb, kstep(ks[a], vs[a], False), st)
                own = i + 1 if causal else f_ref[0] * (n // fb)
                st = lax.fori_loop(0, own, kstep(ks[2], vs[2], causal), st)
                st = lax.fori_loop(0, f_ref[1 if causal else 0] * (n // fb), kstep(ks[3], vs[3], False), st)
                finish(st[1], st[2], st[0], qs)
                return 0

            lax.fori_loop(0, tq // fb, qblock, 0)

    kspec = lambda rows: pl.BlockSpec((rows, d), lambda h, f: (0, h + h0))
    rows = [c, c, n, n]
    keys = 2 * c + n
    return pl.pallas_call(
        kern,
        grid_spec=pltpu.PrefetchScalarGridSpec(
            num_scalar_prefetch=1,
            grid=(nh,),
            in_specs=[pl.BlockSpec((tq, d), lambda h, f: (0, h + qcol))] + [kspec(r) for r in rows] * 2,
            out_specs=[pl.BlockSpec((d, tq), lambda h, f: (h, 0)), pl.BlockSpec((1, 1, tq), lambda h, f: (h, 0, 0))],
            scratch_shapes=[pltpu.VMEM((d, tq), F32), pltpu.VMEM((8, tq), F32)],
        ),
        out_shape=[jax.ShapeDtypeStruct((nh * d, tq), F32), jax.ShapeDtypeStruct((nh, 1, tq), F32)],
        compiler_params=pltpu.CompilerParams(vmem_limit_bytes=VMEM),
        cost_estimate=pl.CostEstimate(flops=12 * tq * keys * nh * d, bytes_accessed=4 * keys * nh * d,
                                      transcendentals=tq * keys * nh),
    )(flags, q, *[kv[0] for kv in kvs], *[kv[1] for kv in kvs])


def _merge(loc, first, rem, nh, d, per=4):
    tq = loc[0].shape[1]
    sizes = [l.shape[0] // per for _, l in rem]
    starts = [sum(sizes[:i]) for i in range(len(sizes))]

    def kern(o1_ref, l1_ref, *refs):
        o_ref = refs[-1]
        h = pl.program_id(0)

        def one(o2_ref, l2_ref):
            for i in range(per):
                rows = slice(i * d, (i + 1) * d)
                a, b = l1_ref[i], l2_ref[i]
                m = jnp.maximum(a, b)
                wa, wb = jnp.exp2(a - m), jnp.exp2(b - m)
                t = 1.0 / (wa + wb)
                o_ref[:, rows] = (o1_ref[rows, :] * (wa * t) + o2_ref[rows, :] * (wb * t)).astype(BF16).T

        for i, (s, n) in enumerate(zip(starts, sizes)):
            pl.when((h >= s) & (h < s + n))(functools.partial(one, refs[2 * i], refs[2 * i + 1]))

    f0 = first // per
    in_specs = [pl.BlockSpec((per * d, tq), lambda h: (h + f0, 0)), pl.BlockSpec((per, 1, tq), lambda h: (h + f0, 0, 0))]
    for s, n in zip(starts, sizes):
        at = lambda h, s=s, n=n: jnp.clip(h - s, 0, n - 1)
        in_specs += [pl.BlockSpec((per * d, tq), lambda h, at=at: (at(h), 0)),
                     pl.BlockSpec((per, 1, tq), lambda h, at=at: (at(h), 0, 0))]
    return pl.pallas_call(
        kern,
        grid=(nh // per,),
        in_specs=in_specs,
        out_specs=pl.BlockSpec((tq, per * d), lambda h: (0, h)),
        out_shape=jax.ShapeDtypeStruct((tq, nh * d), BF16),
        compiler_params=pltpu.CompilerParams(vmem_limit_bytes=VMEM),
        cost_estimate=pl.CostEstimate(flops=2000 * tq * nh * d, bytes_accessed=10 * tq * nh * d, transcendentals=0),
    )(*loc, *[a for r in rem for a in r])


def _flatten(a, b, br=256):
    n, h, d = a.shape

    def kern(a_ref, b_ref, oa_ref, ob_ref):
        oa_ref[...] = a_ref[...].reshape(br, h * d)
        ob_ref[...] = b_ref[...].reshape(br, h * d)

    return pl.pallas_call(
        kern,
        grid=(n // br,),
        in_specs=[pl.BlockSpec((br, h, d), lambda i: (i, 0, 0))] * 2,
        out_specs=[pl.BlockSpec((br, h * d), lambda i: (i, 0))] * 2,
        out_shape=[jax.ShapeDtypeStruct((n, h * d), BF16)] * 2,
        compiler_params=pltpu.CompilerParams(vmem_limit_bytes=52 * 1024 * 1024),
        cost_estimate=pl.CostEstimate(flops=1000 * n * h * d, bytes_accessed=8 * n * h * d, transcendentals=0),
    )(a, b)


def _out(t, terms, halves, acc, ncols, final, bn=512):
    tl = terms[0][0].shape[0]
    nb = ncols // bn
    half = halves[0].shape[0]
    ospec = pl.BlockSpec((tl, bn), lambda j, tt: (0, j))
    args, in_specs, used = [], [], []
    for o, w, row, own in terms:
        rows = o.shape[1]
        args.append(o)
        in_specs.append(pl.BlockSpec(o.shape, lambda j, tt: (0, 0)))
        if own:
            args.append(w)
            in_specs.append(pl.BlockSpec((rows, bn), lambda j, tt, at=row // rows: (at, j + tt[0] * nb)))
            used.append(None)
        else:
            args += halves
            in_specs += [pl.BlockSpec((rows, bn), lambda j, tt, at=row % half // rows: (at, j))] * 2
            used.append(row // half)
    if acc is not None:
        args.append(acc)
        in_specs.append(ospec)

    def kern(t_ref, *refs):
        o_ref = refs[-1]
        r = None if acc is None else refs[-2][...]
        at = 0
        for u in used:
            w = refs[at + 1][...] if u is None else jnp.where(t_ref[1] == u, refs[at + 1][...], refs[at + 2][...])
            p = jnp.dot(refs[at][...], w, preferred_element_type=F32)
            r = p if r is None else r + p
            at += 2 if u is None else 3
        o_ref[...] = r.astype(o_ref.dtype)

    k = sum(o.shape[1] for o, *_ in terms)
    return pl.pallas_call(
        kern,
        grid_spec=pltpu.PrefetchScalarGridSpec(num_scalar_prefetch=1, grid=(nb,), in_specs=in_specs, out_specs=ospec),
        out_shape=jax.ShapeDtypeStruct((tl, ncols), BF16 if final else F32),
        compiler_params=pltpu.CompilerParams(vmem_limit_bytes=VMEM),
        cost_estimate=pl.CostEstimate(flops=2 * tl * k * ncols, bytes_accessed=2 * k * ncols, transcendentals=0),
    )(t, *args)


def solution(mesh):
    ncp = mesh.shape['cp']
    ntp = mesh.shape['tp']
    row = P(('dp', 'cp'), None)
    cache = P(('dp', 'cp'), 'tp', None)
    col = P(None, 'tp')
    half = ncp // 2
    core = [(i, i ^ 1) for i in range(ncp)]
    chip = [(i, (i + half) % ncp) for i in range(ncp)]
    swap = [(0, 1), (1, 0)]

    def body(x, kc, vc, wq, wk, wv, wo):
        tl = x.shape[0]
        cl, hl, d = kc.shape
        w = hl * d
        r = lax.axis_index('cp')
        t = lax.axis_index('tp')
        flags = jnp.stack([(r < half).astype(jnp.int32), r % 2])
        tt = jnp.stack([t, r % 2])
        ncols = wo.shape[1] // ntp
        hq = hl // 2

        def send(a, axis, perm):
            return lax.ppermute(a, axis, perm)

        tabs = _tables(cl * ncp + r * tl + jnp.arange(tl, dtype=jnp.int32), d)
        qs, qr = [], []
        prev = tabs[0]
        for i in range(2):
            qs.append(_proj(x, _after(wq, prev), tabs, i * (w // 2), w // 2, d))
            prev = qs[i]
            qr.append(send(prev, 'cp', chip))
        kc2, vc2 = _flatten(_after(kc, prev), vc)
        kcp = send(kc2, 'cp', core)
        vcp = send(vc2, 'cp', core)
        k = _proj(x, _after(wk, vc2), tabs, 0, w, d)
        kp = send(k, 'cp', core)
        v = _proj(x, _after(wv, k), None, 0, w, d)
        vp = lax.ppermute(v, 'cp', core)
        wo_half = send(lax.dynamic_slice(_after(wo, v), (r % 2 * (w // 2), (1 - t) * ncols), (w // 2, ncols)), 'tp', swap)
        wo_other = [wo_half]
        kvs = [(kc2, vc2), (kcp, vcp), (k, v), (kp, vp)]

        prev, y = v, None
        rem, loc, os = {}, {}, {}
        for kind, h0, nh in ORDER:
            if kind == 'R':
                o, l = _attend(_after(flags, prev), qr[h0 // hq], h0 % hq, kvs, h0, nh, d, False)
                prev = l
            elif kind == 'L':
                loc[h0, nh] = _attend(_after(flags, prev), qs[h0 // hq], h0 % hq, kvs, h0, nh, d, True)
                prev = loc[h0, nh][1]
            elif kind == 'M':
                (l0, ln), part = next((k, p) for k, p in loc.items() if k[0] <= h0 < sum(k))
                prev = _merge((part[0], _after(part[1], prev)), h0 - l0,
                              [rem[g] for g in sorted(rem) if h0 <= g < h0 + nh], nh, d)
                os[h0] = [(prev, wo, h0 * d, True)]
                if h0 + nh == hl:
                    v3 = _after(v, prev).reshape(tl, hl, d)
                if len(wo_other) == 1:
                    wo_other.append(send(_after(wo_half, prev), 'cp', core))
            else:
                terms = sum([os[g] for g in sorted(os) if h0 <= g < h0 + nh], [])
                prev = y = _out(_after(tt, prev), terms, wo_other, y, ncols, kind == 'Z')
            if kind == 'R':
                rem[h0] = send(o, 'cp', chip), send(l, 'cp', chip)
            elif kind == 'M':
                os[h0].append((send(prev, 'tp', swap), None, h0 * d, False))
        return y, k.reshape(tl, hl, d), v3

    return jax.shard_map(body, mesh=mesh,
                         in_specs=(row, cache, cache, col, col, col, P('tp', None)),
                         out_specs=(P(('dp', 'cp'), 'tp'), cache, cache), check_vma=False)
```
